256 devices in a mesh: var: 32 (over y, x, core), tp: 8 (over z).
Axes of the slice: x: 4, y: 4, z: 8, core: 2. Of those that a mesh axis runs over, the one named last changes fastest.
Arguments:
- tokens: bfloat16 [32768, 8192], P('var', 'tp'), may hold values from -6 to 6
- kv_weight: bfloat16 [8192, 2048], P('tp'), may hold values from -0.0625 to 0.0625
- factor_a: bfloat16 [64, 8192, 128], P('var', 'tp'), may hold values from -0.0625 to 0.0625
- factor_scale: bfloat16 [64, 128], P('var'), may hold values from 0.29882812 to 3
- factor_b: bfloat16 [64, 128, 2048], P('var', None, 'tp'), may hold values from -0.5 to 0.5
- counts: int32 [32, 64], replicated, may hold values from 0 to 64, as said below
Outputs:
- kv_out: bfloat16 [32768, 2048], P('var', 'tp')
The draws below stay inside these ranges and needn't reach their ends.
Inputs may be any that keep to these rules, and one draw needn't show every extreme that they name: `counts`: each row sums to 1024. Owner o holds variants 2 * o to 2 * o + 1; in every row those variants together have at most 64 tokens, and in every draw one owner has exactly 64 tokens in every row.
All inputs are finite; a program needn't handle non-finite values.
Results may differ from the reference program's by a relative error of at most 0.011.
Values may be sent and summed in bfloat16 or wider, within the bound.
No kernel may reach another device: no remote copies, remote signals or barrier semaphores. Data moves between devices by JAX's collectives and lax.ppermute only.
A program may use at most 128 MiB of HBM per device.

```python
import math
import jax
import jax.numpy as jnp
from jax import lax

D = 8192
R = 128
VAR_DEV = 2
TOK_GRP = 1024
KVW = 2048
GROUPS = 32
VARIANTS = 64
CAP = 64
TOKENS = 32768


def draw_counts(key, part):
    folded = jax.random.fold_in(key, 7)
    subkeys = jax.random.split(folded, 5)
    popular = jax.random.permutation(subkeys[0], GROUPS)
    orders = jax.vmap(lambda subkey: jax.random.permutation(subkey, GROUPS))(jax.random.split(subkeys[1], GROUPS))
    pair_count = GROUPS // 2
    first_owner = orders[:, 0::2]
    second_owner = orders[:, 1::2]
    pop_first = popular[first_owner]
    pop_second = popular[second_owner]
    draw_one = jax.random.randint(subkeys[2], (GROUPS, pair_count), 0, CAP + 1)
    draw_two = jax.random.randint(subkeys[3], (GROUPS, pair_count), 0, CAP + 1)
    strong = jnp.maximum(draw_one, draw_two)
    first_share = jnp.where(pop_first > pop_second, strong, CAP - strong)
    first_share = jnp.where(pop_first == GROUPS - 1, CAP, first_share)
    first_share = jnp.where(pop_second == GROUPS - 1, 0, first_share)
    row_ids = jnp.arange(GROUPS)[:, None]
    owner_loads = jnp.zeros((GROUPS, GROUPS), jnp.int32)
    owner_loads = owner_loads.at[row_ids, first_owner].set(first_share.astype(jnp.int32))
    owner_loads = owner_loads.at[row_ids, second_owner].set((CAP - first_share).astype(jnp.int32))
    first_part = jax.random.randint(subkeys[4], (GROUPS, GROUPS), 0, owner_loads + 1)
    forced = (row_ids == 0) & (popular[None, :] == GROUPS - 1)
    first_part = jnp.where(forced, owner_loads, first_part)
    split_counts = jnp.stack([first_part, owner_loads - first_part], axis=2)
    return split_counts.reshape(GROUPS, VARIANTS).astype(jnp.int32)


def block_levels(own_key, shape, cuts, smallest, top_value):
    loudness, own = 1.0, jax.random.fold_in(own_key, 6)
    for dim, shards_of in cuts:
        draws = jnp.exp(jax.random.uniform(jax.random.fold_in(own, dim), (shards_of,), jnp.float32, smallest / len(cuts), top_value / len(cuts)))
        loudness = loudness * jnp.repeat(draws, shape[dim] // shards_of).reshape([-1 if axis == dim else 1 for axis in range(len(shape))])
    return loudness


def noise(key, shape, spread, most, cuts=(), kind=jnp.bfloat16):
    array = spread * jax.random.normal(key, shape, jnp.float32)
    if cuts:
        array = array * block_levels(key, shape, cuts, -0.22, 0.18)
    return jnp.clip(array, -most, most).astype(kind)


def setup_inputs(seed: int = 0) -> dict:
    keys = jax.random.split(jax.random.key(seed), 7)
    tokens = noise(keys[0], (TOKENS, D), 1.0, 6.0, ((0, 32), (1, 8)))
    kv_weight = noise(keys[1], (D, KVW), D ** -0.5, 0.0625, ((0, 8),))
    factor_a = noise(keys[2], (VARIANTS, D, R), D ** -0.5, 0.0625, ((0, 32), (1, 8)))
    factor_scale = jnp.clip(jnp.exp(math.log(3.0) - 2.306499 * jax.random.uniform(keys[3], (VARIANTS, R), jnp.float32) ** block_levels(keys[3], (VARIANTS, R), ((0, 32),), -0.2, 0.2)), 0.29882812, 3.0).astype(jnp.bfloat16)
    factor_b = noise(keys[4], (VARIANTS, R, KVW), R ** -0.5, 0.5, ((0, 32), (2, 8)))
    counts = draw_counts(jax.random.fold_in(keys[6], 71), 0)
    return {"tokens": tokens, "kv_weight": kv_weight, "factor_a": factor_a, "factor_scale": factor_scale, "factor_b": factor_b, "counts": counts}


def owner_layout(group_counts):
    owner_counts = group_counts.reshape(GROUPS, VAR_DEV)
    starts = jnp.cumsum(group_counts) - group_counts
    first_rows = starts.reshape(GROUPS, VAR_DEV)[:, 0]
    slot_ids = jnp.arange(CAP, dtype=jnp.int32)
    filled = jnp.sum(owner_counts, axis=1)
    inside = slot_ids[None, :] < filled[:, None]
    bounds = jnp.cumsum(owner_counts, axis=1)
    local_pick = jnp.sum((slot_ids[None, :, None] >= bounds[:, None, :VAR_DEV - 1]).astype(jnp.int32), axis=2)
    picker = (local_pick[:, :, None] == jnp.arange(VAR_DEV, dtype=jnp.int32)[None, None, :]).astype(jnp.float32)
    return first_rows, inside, picker


def reference(tokens, kv_weight, factor_a, factor_scale, factor_b, counts):
    base_part = jnp.dot(tokens, kv_weight, preferred_element_type=jnp.float32)
    factor_in = factor_a.astype(jnp.float32).reshape(GROUPS, VAR_DEV, D, R)
    factor_out = factor_b.astype(jnp.float32).reshape(GROUPS, VAR_DEV, R, KVW)
    scale_table = factor_scale.astype(jnp.float32).reshape(GROUPS, VAR_DEV, R)[:, None]
    grouped = tokens.reshape(GROUPS, TOK_GRP, D)

    def one_group(inputs):
        group_tokens, group_counts = inputs
        first_rows, inside, picker = owner_layout(group_counts)
        slot_ids = jnp.arange(CAP, dtype=jnp.int32)
        row_index = jnp.clip(first_rows[:, None] + slot_ids[None, :], 0, TOK_GRP - 1).astype(jnp.int32)
        gathered = jnp.where(inside[:, :, None], group_tokens[row_index], jnp.zeros((), group_tokens.dtype))
        gathered = gathered.astype(jnp.float32)
        products = jnp.einsum("ocd,ovdr->ocvr", gathered, factor_in)
        rank_total = jnp.sum(products * picker[..., None], axis=2)
        scaled = rank_total * jnp.sum(picker[..., None] * scale_table, axis=2)
        scaled = lax.optimization_barrier(scaled.astype(jnp.bfloat16)).astype(jnp.float32)
        outputs = jnp.einsum("ocr,ovrk->ocvk", scaled, factor_out)
        delta_blocks = jnp.sum(outputs * picker[..., None], axis=2).astype(jnp.bfloat16)
        ends_at = jnp.cumsum(group_counts)
        position = jnp.arange(TOK_GRP, dtype=jnp.int32)
        variant = jnp.sum((ends_at[None, :] <= position[:, None]).astype(jnp.int32), axis=1)
        owner_of = variant // VAR_DEV
        owner_hot = owner_of[:, None] == jnp.arange(GROUPS, dtype=jnp.int32)[None, :]
        owner_first = jnp.sum(jnp.where(owner_hot, first_rows[None, :], 0), axis=1)
        flat_index = (owner_of * CAP + position - owner_first).astype(jnp.int32)
        return delta_blocks.reshape(GROUPS * CAP, KVW)[flat_index]

    delta_rows = lax.map(one_group, (grouped, counts)).reshape(TOKENS, KVW)
    return (base_part + delta_rows.astype(jnp.float32)).astype(jnp.bfloat16)
```

```python
import functools

import jax
import jax.numpy as jnp
from jax import lax
from jax.experimental import pallas as pl
from jax.experimental.pallas import tpu as pltpu
from jax.sharding import PartitionSpec as P


SIDE = 4
CORES = 2
WINDOW = 80


def ring(first_axis, step):
    pairs = []
    for y in range(SIDE):
        for x in range(SIDE):
            for c in range(CORES):
                along_x = (c == 0) == first_axis
                ty, tx = (y, (x + step) % SIDE) if along_x else ((y + step) % SIDE, x)
                pairs.append(((y * SIDE + x) * CORES + c, (ty * SIDE + tx) * CORES + c))
    return pairs


def shift(value, first_axis, step):
    return lax.ppermute(value, "var", ring(first_axis, step))


def swap_cores(value):
    return lax.ppermute(value, "var", [(v, v ^ 1) for v in range(SIDE * SIDE * CORES)])


def owner_bounds(bounds, group, owner):
    return bounds[group, 2 * owner], bounds[group, 2 * owner + 1], bounds[group, 2 * owner + 2]


def window_of(start, rows):
    return pl.multiple_of(jnp.minimum((start // 16) * 16, rows - WINDOW), 16)


def rank_kernel(slots, n_factors, has_prev, bounds, owners, own_tok, sib_tok, *rest):
    factors = rest[:n_factors]
    out = rest[-1]
    tokens = (own_tok, sib_tok)
    rows_all = own_tok.shape[0]
    out[...] = rest[n_factors][...] if has_prev else jnp.zeros_like(out)
    for place, first, second in slots:
        owner = owners[place]
        both = jnp.concatenate([factors[first[0]][first[1]], factors[second[0]][second[1]]], axis=1)
        marks = [owner_bounds(bounds, g, owner) for g in range(2)]
        bases = [window_of(marks[g][0], rows_all) for g in range(2)]
        lhs = jnp.concatenate([tokens[g][pl.ds(bases[g], WINDOW), :] for g in range(2)], axis=0)
        products = jnp.dot(lhs, both, preferred_element_type=jnp.float32)
        rank = both.shape[1] // 2
        for g in range(2):
            start, middle, end = marks[g]
            part = products[g * WINDOW : (g + 1) * WINDOW]
            rows = bases[g] + lax.broadcasted_iota(jnp.int32, (WINDOW, rank), 0)
            picked = jnp.where(rows < middle, part[:, :rank], part[:, rank:])
            here = out[g, pl.ds(bases[g], WINDOW), :].astype(jnp.float32)
            inside = (rows >= start) & (rows < end)
            out[g, pl.ds(bases[g], WINDOW), :] = jnp.where(inside, picked, here).astype(out.dtype)


def rank_part(slots, bounds, owners, tokens, factors, prev):
    rows, width = tokens[0].shape
    rank = factors[0].shape[-1]
    smem = pl.BlockSpec(memory_space=pltpu.SMEM)
    vmem = pl.BlockSpec(memory_space=pltpu.VMEM)
    extra = [] if prev is None else [prev]
    return pl.pallas_call(
        functools.partial(rank_kernel, slots, len(factors), prev is not None),
        out_shape=jax.ShapeDtypeStruct((2, rows, rank), jnp.bfloat16),
        in_specs=[smem, smem] + [vmem] * (2 + len(factors) + len(extra)),
        out_specs=vmem,
        compiler_params=pltpu.CompilerParams(vmem_limit_bytes=24 * 1024 * 1024),
        cost_estimate=pl.CostEstimate(
            flops=2 * 2 * WINDOW * len(slots) * width * 2 * rank, bytes_accessed=8 << 20, transcendentals=0
        ),
    )(bounds, owners, *tokens, *factors, *extra)


def combine_kernel(n_owners, bounds, scaled, factor, base, out):
    rows_all, cols = out.shape
    rank = scaled.shape[1]

    def one_owner(owner, carry):
        start, middle, end = owner_bounds(bounds, 0, owner)
        first = window_of(start, rows_all)
        rows = first + lax.broadcasted_iota(jnp.int32, (WINDOW, rank), 0)
        values = scaled[pl.ds(first, WINDOW), :].astype(jnp.float32)
        lhs = jnp.concatenate(
            [
                jnp.where((rows >= start) & (rows < middle), values, 0.0),
                jnp.where((rows >= middle) & (rows < end), values, 0.0),
            ],
            axis=1,
        ).astype(jnp.bfloat16)
        rhs = factor[pl.ds(2 * owner, 2)].reshape(2 * rank, cols)
        delta = jnp.dot(lhs, rhs, preferred_element_type=jnp.float32)
        delta = delta.astype(jnp.bfloat16).astype(jnp.float32)
        total = base[pl.ds(first, WINDOW), :].astype(jnp.float32) + delta
        row_ids = first + lax.broadcasted_iota(jnp.int32, (WINDOW, cols), 0)
        here = out[pl.ds(first, WINDOW), :].astype(jnp.float32)
        inside = (row_ids >= start) & (row_ids < end)
        out[pl.ds(first, WINDOW), :] = jnp.where(inside, total, here).astype(out.dtype)
        return carry

    lax.fori_loop(0, n_owners, one_owner, 0)


def combine(bounds, scaled, factor, base):
    smem = pl.BlockSpec(memory_space=pltpu.SMEM)
    vmem = pl.BlockSpec(memory_space=pltpu.VMEM)
    n_owners = factor.shape[0] // 2
    return pl.pallas_call(
        functools.partial(combine_kernel, n_owners),
        out_shape=jax.ShapeDtypeStruct(base.shape, jnp.bfloat16),
        in_specs=[smem, vmem, vmem, vmem],
        out_specs=vmem,
        compiler_params=pltpu.CompilerParams(vmem_limit_bytes=16 * 1024 * 1024),
        cost_estimate=pl.CostEstimate(
            flops=2 * WINDOW * n_owners * 2 * scaled.shape[1] * base.shape[1], bytes_accessed=6 << 20, transcendentals=0
        ),
    )(bounds, scaled, factor, base)


def collected_owners(position):
    core = position % CORES
    y, x = position // (SIDE * CORES), (position // CORES) % SIDE
    place = jnp.arange(16, dtype=jnp.int32)
    first_off = place % 4 + 3
    group = place // 4
    second_off = jnp.where(group == 0, 0, jnp.where(group == 1, 3, jnp.where(group == 2, 1, 2)))
    x_off = jnp.where(core == 0, first_off, second_off)
    y_off = jnp.where(core == 0, second_off, first_off)
    return (((y + y_off) % SIDE) * SIDE + (x + x_off) % SIDE) * CORES + core


def body(tokens, kv_weight, factor_a, factor_scale, factor_b, counts):
    position = lax.axis_index("var")
    tp_size = lax.axis_size("tp")
    rows = tokens.shape[0]
    variants = counts.shape[1]

    scaled_a = (factor_a.astype(jnp.float32) * factor_scale.astype(jnp.float32)[:, None, :]).astype(jnp.bfloat16)
    left = shift(scaled_a, True, 1)
    right = shift(scaled_a, True, -1)
    sib_tokens = swap_cores(tokens)

    partial_value = jnp.dot(tokens, kv_weight, preferred_element_type=jnp.float32).astype(jnp.bfloat16)
    base = lax.psum_scatter(partial_value, "tp", scatter_dimension=1, tiled=True)
    every_b = lax.all_gather(factor_b, "var", axis=0, tiled=True)

    pair = jnp.stack([position, position ^ 1])
    pair_counts = counts[pair]
    ids = jnp.arange(128, dtype=jnp.int32)
    before = jnp.arange(variants, dtype=jnp.int32)[None, None, :] < ids[None, :, None]
    bounds = jnp.sum(jnp.where(before, pair_counts[:, None, :], 0), axis=2)
    owners = collected_owners(position)

    near = jnp.concatenate([left, scaled_a, right], axis=0)
    far = jnp.concatenate([shift(left[0:1], True, 1), shift(right[1:2], True, -1)], axis=0)
    near_m, near_p = shift(near, False, 1), shift(near, False, -1)
    far_m, far_p = shift(far, False, 1), shift(far, False, -1)
    near_d, near_e = shift(near_m[0:3], False, 1), shift(near_p[3:6], False, -1)
    far_d, far_e = shift(far_m[0:1], False, 1), shift(far_p[1:2], False, -1)

    toks = (tokens, sib_tokens)
    three = lambda place, arr: [(place + k, (arr, 2 * k), (arr, 2 * k + 1)) for k in range(3)]
    one = lambda place, arr: [(place, (arr, 0), (arr, 1))]
    ranks = rank_part(three(0, 0) + one(3, 1), bounds, owners, toks, [near, far], None)
    ranks = rank_part(three(4, 0) + three(8, 1), bounds, owners, toks, [near_m, near_p], ranks)
    last = one(7, 0) + one(11, 1) + [
        (12, (2, 0), (2, 1)),
        (13, (2, 2), (3, 0)),
        (14, (3, 1), (3, 2)),
        (15, (4, 0), (5, 0)),
    ]
    ranks = rank_part(last, bounds, owners, toks, [far_m, far_p, near_d, near_e, far_d, far_e], ranks)

    mine = ranks[0] + swap_cores(ranks[1])
    parts = lax.all_to_all(mine.reshape(tp_size, rows // tp_size, -1), "tp", 0, 0, tiled=True)
    share = jnp.sum(parts.astype(jnp.float32), axis=0).astype(jnp.bfloat16)
    copies = jnp.broadcast_to(share, (tp_size, *share.shape))
    scaled = lax.all_to_all(copies, "tp", 0, 0, tiled=True).reshape(rows, -1)
    return combine(bounds, scaled, every_b, base)


def solution(mesh):
    return jax.shard_map(
        body,
        mesh=mesh,
        in_specs=(
            P("var", "tp"),
            P("tp", None),
            P("var", "tp", None),
            P("var", None),
            P("var", None, "tp"),
            P(),
        ),
        out_specs=P("var", "tp"),
        check_vma=False,
    )
```
